32 devices in a mesh: pose: 8 (over z, x), rank: 4 (over y, core).
Axes of the slice: x: 2, y: 2, z: 4, core: 2. Of those that a mesh axis runs over, the one named last changes fastest.
Arguments:
- initial: float32 [4, 3, 131072], P(None, None, ('pose', 'rank')), may hold values from -0.12 to 1.12, as said below
- right_rot: float32 [3, 3, 131072], P(None, None, ('pose', 'rank')), may hold values from -1 to 1, as said below
- right_wt: float32 [131072], P(('pose', 'rank')), may hold values from 0.3 to 3
- down_rot: float32 [3, 3, 131072], P(None, None, ('pose', 'rank')), may hold values from -1 to 1, as said below
- down_wt: float32 [131072], P(('pose', 'rank')), may hold values from 0.3 to 3
- loop_ends: int32 [2, 65536], P(None, ('pose', 'rank')), may hold values from 0 to 4095
- loop_rot: float32 [3, 3, 65536], P(None, None, ('pose', 'rank')), may hold values from -1 to 1, as said below
- loop_wt: float32 [65536], P(('pose', 'rank')), may hold values from 0.3 to 3
- step_sizes: float32 [2], replicated, may hold values from 0.03 to 0.08
Outputs:
- poses_out: float32 [4, 3, 131072], P(None, None, ('pose', 'rank'))
- costs: float32 [3], replicated
The draws below stay inside these ranges and needn't reach their ends.
Inputs may be any that keep to these rules, and one draw needn't show every extreme that they name: `right_rot`: every 3 x 3 block is a rotation matrix. `down_rot`: every 3 x 3 block is a rotation matrix. `loop_rot`: every 3 x 3 block is a rotation matrix. `initial`: every entry differs from the same entry of the first three columns of the 4 x 4 identity by at most 0.12.
All inputs are finite; a program needn't handle non-finite values.
Results may differ from the reference program's by a relative error of at most 0.0001.
Values sent between devices are 32-bit elements; how exact they have to be, the bound alone decides.
A program may use at most 64 MiB of HBM per device.

```python
import math
import jax
import jax.numpy as jnp
from jax import lax

P_SIZE = 4
DIM = 3
ROWS_DEV = 4
COLS = 1024
LOOPS_DEV = 2048
ITERS = 2
POSE_DEV = 4096
POSES = 131072
ROWS = 128
LOOPS = 65536
N_POSE = 8
N_RANK = 4


def rotations(key, number, spread):
    axis_vec = jax.random.normal(key, (3, number), jnp.float32) * spread
    angle_size = jnp.sqrt(jnp.sum(axis_vec * axis_vec, 0) + 1e-12)
    unit = axis_vec / angle_size
    zeros_row = jnp.zeros((number,), jnp.float32)
    skew = jnp.stack([jnp.stack([zeros_row, -unit[2], unit[1]]), jnp.stack([unit[2], zeros_row, -unit[0]]), jnp.stack([-unit[1], unit[0], zeros_row])])
    skew_sq = jnp.sum(skew[:, :, None, :] * skew[None, :, :, :], axis=1)
    identity = jnp.eye(3, dtype=jnp.float32)[:, :, None]
    return identity + jnp.sin(angle_size) * skew + (1.0 - jnp.cos(angle_size)) * skew_sq


def draw_right_rot(key, part):
    spread = 0.5
    return rotations(jax.random.fold_in(key, 11), POSES, spread)


def draw_down_rot(key, part):
    spread = 0.5
    return rotations(jax.random.fold_in(key, 12), POSES, spread)


def draw_loop_rot(key, part):
    spread = 0.5
    return rotations(jax.random.fold_in(key, 13), LOOPS, spread)


def draw_initial(key, part):
    sub = jax.random.fold_in(key, 14)
    noise = jnp.clip(0.05 * jax.random.normal(sub, (P_SIZE, DIM, POSES), jnp.float32), -0.12, 0.12)
    return jnp.eye(P_SIZE, DIM, dtype=jnp.float32)[:, :, None] + noise


def with_ends(values, key, smallest, high):
    shape = values.shape
    spot = [jax.random.randint(jax.random.fold_in(key, axis), (), 0, shape[axis]) for axis in range(len(shape))]
    values = values.at[tuple(spot)].set(smallest)
    longest = shape.index(max(shape))
    spot[longest] = (spot[longest] + 1) % shape[longest]
    return values.at[tuple(spot)].set(high)


def block_levels(key, dims, split, low, high):
    factor_of = 1.0
    for position, blocks in split:
        heights = jax.random.uniform(jax.random.fold_in(jax.random.fold_in(key, 6), position), (blocks,), jnp.float32, low / len(split), high / len(split))
        factor_of = factor_of * jnp.repeat(jnp.exp(heights), dims[position] // blocks).reshape((-1,) + (1,) * (len(dims) - 1 - position))
    return factor_of


def setup_inputs(seed: int = 0) -> dict:
    key_list = jax.random.split(jax.random.key(seed), 10)
    return {
        "initial": draw_initial(jax.random.fold_in(key_list[9], 71), 0),
        "right_rot": draw_right_rot(jax.random.fold_in(key_list[9], 71), 0),
        "right_wt": jnp.clip(jnp.exp(math.log(3.0) - 2.3025851 * jax.random.uniform(key_list[2], (POSES,), jnp.float32) ** block_levels(key_list[2], (POSES,), ((0, 32),), -0.2, 0.2)), 0.3, 3.0),
        "down_rot": draw_down_rot(jax.random.fold_in(key_list[9], 71), 0),
        "down_wt": jnp.clip(jnp.exp(math.log(3.0) - 2.3025851 * jax.random.uniform(key_list[4], (POSES,), jnp.float32) ** block_levels(key_list[4], (POSES,), ((0, 32),), -0.2, 0.2)), 0.3, 3.0),
        "loop_ends": with_ends(jax.random.randint(key_list[5], (2, LOOPS), 0, ROWS_DEV * COLS), jax.random.fold_in(key_list[5], 1), 0, (ROWS_DEV * COLS) - 1).astype(jnp.int32),
        "loop_rot": draw_loop_rot(jax.random.fold_in(key_list[9], 71), 0),
        "loop_wt": jnp.clip(jnp.exp(math.log(3.0) - 2.3025851 * jax.random.uniform(key_list[7], (LOOPS,), jnp.float32) ** block_levels(key_list[7], (LOOPS,), ((0, 32),), -0.2, 0.2)), 0.3, 3.0),
        "step_sizes": jnp.clip(jax.random.uniform(key_list[8], (ITERS,), jnp.float32, 0.03, 0.08), 0.03, 0.08),
    }


def rotate(blocks, rot):
    return lax.optimization_barrier(jnp.sum(blocks[:, :, None, :] * rot[None], axis=1))

def rotate_back(blocks, rot):
    return lax.optimization_barrier(jnp.sum(blocks[:, None, :, :] * rot[None], axis=2))

def orthonormal(blocks):
    col_one = blocks[:, 0]
    col_two = blocks[:, 1]
    col_three = blocks[:, 2]
    col_one = col_one / jnp.sqrt(lax.optimization_barrier(jnp.sum(col_one * col_one, 0)))
    col_two = col_two - lax.optimization_barrier(jnp.sum(col_one * col_two, 0)) * col_one
    col_three = col_three - lax.optimization_barrier(jnp.sum(col_one * col_three, 0)) * col_one
    col_two = col_two / jnp.sqrt(lax.optimization_barrier(jnp.sum(col_two * col_two, 0)))
    col_three = col_three - lax.optimization_barrier(jnp.sum(col_two * col_three, 0)) * col_two
    col_three = col_three / jnp.sqrt(lax.optimization_barrier(jnp.sum(col_three * col_three, 0)))
    return jnp.stack([col_one, col_two, col_three], axis=1)

def reference(initial, right_rot, right_wt, down_rot, down_wt, loop_ends, loop_rot, loop_wt, step_sizes):
    band_total = N_POSE * N_RANK
    positions = jnp.arange(POSES)
    right_w = jnp.where(positions % COLS < COLS - 1, right_wt, 0.0)
    down_w = jnp.where(positions // COLS < ROWS - 1, down_wt, 0.0)
    bands = (jnp.arange(LOOPS) // LOOPS_DEV).astype(jnp.int32)
    sources = (bands * POSE_DEV + loop_ends[0]).astype(jnp.int32)
    targets = ((bands + band_total // 2) % band_total * POSE_DEV + loop_ends[1]).astype(jnp.int32)

    def evaluate(blocks):
        err_right = jnp.roll(blocks, -1, axis=2) - rotate(blocks, right_rot)
        err_down = jnp.roll(blocks, -COLS, axis=2) - rotate(blocks, down_rot)
        err_loop = blocks[:, :, targets] - rotate(blocks[:, :, sources], loop_rot)
        weighted_right = right_w * err_right
        weighted_down = down_w * err_down
        weighted_loop = loop_wt * err_loop
        total = jnp.sum(weighted_right * err_right) + jnp.sum(weighted_down * err_down) + jnp.sum(weighted_loop * err_loop)
        gradient = jnp.roll(weighted_right, 1, axis=2) - rotate_back(weighted_right, right_rot)
        gradient = gradient + jnp.roll(weighted_down, COLS, axis=2) - rotate_back(weighted_down, down_rot)
        gradient = gradient.at[:, :, sources].add(-rotate_back(weighted_loop, loop_rot))
        gradient = gradient.at[:, :, targets].add(weighted_loop)
        return (0.5 * total / POSES, gradient)
    blocks = orthonormal(initial)
    costs = []
    for iteration in range(ITERS):
        value, gradient = evaluate(blocks)
        costs.append(value)
        inner = lax.optimization_barrier(jnp.sum(blocks[:, :, None, :] * gradient[:, None, :, :], axis=0))
        sym = 0.5 * (inner + jnp.transpose(inner, (1, 0, 2)))
        tangent = gradient - rotate(blocks, sym)
        blocks = orthonormal(blocks - step_sizes[iteration] * tangent)
    value, gradient = evaluate(blocks)
    costs.append(value)
    return (blocks, jnp.stack(costs).astype(jnp.float32))
```

```python
import functools
import jax
import jax.numpy as jnp
from jax import lax
from jax.experimental import pallas as pl
from jax.experimental.pallas import tpu as pltpu
from jax.sharding import PartitionSpec as P

COLS = 1024
LANES = 128
SUB = COLS // LANES
LIFTED = 4
FRAME = 3
COMPS = LIFTED * FRAME
MESH = pl.DeviceIdType.MESH


def mul_rot(y, rot):
    return [
        sum(y[i * FRAME + a] * rot[a * FRAME + b] for a in range(FRAME))
        for i in range(LIFTED)
        for b in range(FRAME)
    ]


def mul_rot_t(y, rot):
    return [
        sum(y[i * FRAME + b] * rot[a * FRAME + b] for b in range(FRAME))
        for i in range(LIFTED)
        for a in range(FRAME)
    ]


def qf(y):
    cols = [[y[i * FRAME + a] for i in range(LIFTED)] for a in range(FRAME)]

    def unit(col):
        inv = lax.rsqrt(sum(v * v for v in col))
        return [v * inv for v in col]

    def less(col, base):
        along = sum(u * v for u, v in zip(base, col))
        return [v - along * u for u, v in zip(base, col)]

    one = unit(cols[0])
    two = unit(less(cols[1], one))
    three = unit(less(less(cols[2], one), two))
    cols = [one, two, three]
    return [cols[a][i] for i in range(LIFTED) for a in range(FRAME)]


def kernel(
    ranks, poses, scale,
    init, right_rot, right_wt, down_rot, down_wt, ends, loop_rot, loop_wt, steps,
    out_y, out_cost,
    ys, wanted, near_out, near_in, src_rot, src_out, src_in, top_in, last_out, last_in,
    grad, vals, spread, table, sums, red_out, red_rank, red_pose,
    idx_sem, near_sem, src_sem, top_sem, last_sem, rank_sem, pose_sem,
):
    iters = steps.shape[0]
    pose_rows = init.shape[1]
    bands_rows = pose_rows // SUB
    loop_rows = loop_wt.shape[0]
    half_rows = pose_rows // 2
    my_pose = lax.axis_index("pose")
    my_rank = lax.axis_index("rank")
    bands = ranks * poses
    me = my_pose * ranks + my_rank

    def band(flat):
        return (flat // ranks, flat % ranks)

    partner = band((me + bands // 2) % bands)
    above = band((me + bands - 1) % bands)
    below = band((me + 1) % bands)

    barrier = pltpu.get_barrier_semaphore()
    for target in (partner, above, below):
        pl.semaphore_signal(barrier, inc=1, device_id=target, device_id_type=MESH)
    for d in range(1, ranks):
        pl.semaphore_signal(
            barrier, inc=1, device_id=(my_pose, (my_rank + d) % ranks), device_id_type=MESH
        )
    for d in range(1, poses):
        pl.semaphore_signal(
            barrier, inc=1, device_id=((my_pose + d) % poses, my_rank), device_id_type=MESH
        )
    pl.semaphore_wait(barrier, 3 + ranks - 1 + poses - 1)

    def send(src, dst, sems, slot, target):
        copy = pltpu.make_async_remote_copy(
            src_ref=src, dst_ref=dst, send_sem=sems.at[0, slot], recv_sem=sems.at[1, slot],
            device_id=target, device_id_type=MESH,
        )
        copy.start()
        return copy

    idx_copy = send(ends.at[1], wanted, idx_sem, 0, partner)

    lane = lax.broadcasted_iota(jnp.int32, (SUB, LANES), 1)
    sub = lax.broadcasted_iota(jnp.int32, (SUB, LANES), 0)
    row_end = (lane == LANES - 1) & (sub == SUB - 1)
    last_band = me == bands - 1

    def block(ref, v, count, lead=None):
        rows = pl.ds(v * SUB, SUB)
        if lead is None:
            return [ref[c, rows, :] for c in range(count)]
        return [ref[lead, c, rows, :] for c in range(count)]

    def next_col(x):
        x = pltpu.roll(x, LANES - 1, 1)
        return jnp.where(lane == LANES - 1, pltpu.roll(x, SUB - 1, 0), x)

    def prev_col(x):
        x = pltpu.roll(x, 1, 1)
        return jnp.where(lane == 0, pltpu.roll(x, 1, 0), x)

    def gather(t, index):
        row = index // LANES
        col = index % LANES
        rows = index.shape[0]

        def step(r, acc):
            hit = row == r
            new = []
            for c in range(COMPS):
                data = jnp.broadcast_to(ys[t, c, pl.ds(r, 1), :], (rows, LANES))
                got = jnp.take_along_axis(data, col, axis=1, mode="promise_in_bounds")
                new.append(jnp.where(hit, got, acc[c]))
            return tuple(new)

        zero = jnp.zeros((rows, LANES), jnp.float32)
        return lax.fori_loop(0, pose_rows, step, (zero,) * COMPS)

    def fill_table(index_ref, base):
        def step(k, carry):
            index = index_ref[pl.ds(k, 1), :]
            low = (index // (half_rows * LANES)) * LANES + index % LANES
            place = lax.broadcasted_iota(jnp.int32, (2 * LANES, LANES), 0)
            hot = jnp.where(place == low, 1.0, 0.0).astype(jnp.bfloat16)
            table[:, pl.ds(pl.multiple_of((base + k) * LANES, LANES), LANES)] = hot
            return carry

        lax.fori_loop(0, loop_rows, step, 0)

    def scatter(index_ref, values_ref, lead, base):
        def step(k, carry):
            index = index_ref[pl.ds(k, 1), :]
            high = (index // LANES) % half_rows
            hit = lax.broadcasted_iota(jnp.int32, (half_rows, LANES), 0) == high
            at = pl.ds(pl.multiple_of(k * LANES, LANES), LANES)
            for c in range(COMPS):
                if lead is None:
                    value = values_ref[c, pl.ds(k, 1), :]
                else:
                    value = values_ref[lead, c, pl.ds(k, 1), :]
                coarse = value.astype(jnp.bfloat16).astype(jnp.float32)
                fine = value - coarse
                spread[pl.ds(c * half_rows, half_rows), at] = jnp.where(
                    hit, coarse, 0.0
                ).astype(jnp.bfloat16)
                spread[pl.ds((COMPS + c) * half_rows, half_rows), at] = jnp.where(
                    hit, fine, 0.0
                ).astype(jnp.bfloat16)
            return carry

        lax.fori_loop(0, loop_rows, step, 0)
        span = loop_rows * LANES
        placed = lax.dot_general(
            spread[...], table[:, base * LANES : base * LANES + span],
            (((1,), (1,)), ((), ())), preferred_element_type=jnp.float32,
        )
        for c in range(COMPS):
            both = (
                placed[c * half_rows : (c + 1) * half_rows]
                + placed[(COMPS + c) * half_rows : (COMPS + c + 1) * half_rows]
            )
            for h in range(2):
                grad[c, h * half_rows : (h + 1) * half_rows, :] += both[
                    :, h * LANES : (h + 1) * LANES
                ]

    def first(v, carry):
        new = qf(block(init, v, COMPS))
        for c in range(COMPS):
            ys[0, c, pl.ds(v * SUB, SUB), :] = new[c]
        return carry

    lax.fori_loop(0, bands_rows, first, 0)
    fill_table(ends.at[0], 0)
    for t in range(iters + 1):
        need_grad = t < iters
        top_copy = send(ys.at[t, :, pl.ds(0, SUB), :], top_in.at[t], top_sem, t, above)
        if t == 0:
            idx_copy.wait()
        got = gather(t, wanted[...])
        for c in range(COMPS):
            near_out[t, c] = got[c]
        near_copy = send(near_out.at[t], near_in.at[t], near_sem, t, partner)
        end_rows = pl.ds((bands_rows - 1) * SUB, SUB)
        if need_grad:
            rot = block(down_rot, bands_rows - 1, FRAME * FRAME)
            weight = jnp.where(last_band, 0.0, down_wt[end_rows, :])
            turned = mul_rot(block(ys, bands_rows - 1, COMPS, t), rot)
            for c in range(COMPS):
                last_out[t, c] = weight * turned[c]
            last_copy = send(last_out.at[t], last_in.at[t], last_sem, t, below)
        got = gather(t, ends[0])
        turned = mul_rot(got, [loop_rot[k] for k in range(FRAME * FRAME)])
        for c in range(COMPS):
            src_rot[c] = turned[c]
        if need_grad:
            for c in range(COMPS):
                src_out[t, c] = loop_wt[...] * turned[c]
            src_copy = send(src_out.at[t], src_in.at[t], src_sem, t, partner)
        if t == 0:
            fill_table(wanted, loop_rows)

        def add_cost(weight, err):
            sums[t] += weight * sum(e * e for e in err)

        sums[t] = jnp.zeros((SUB, LANES), jnp.float32)

        def right_edges(v, carry):
            here = block(ys, v, COMPS, t)
            rot = block(right_rot, v, FRAME * FRAME)
            weight = jnp.where(row_end, 0.0, right_wt[pl.ds(v * SUB, SUB), :])
            ahead = [next_col(x) for x in here]
            moved = mul_rot(here, rot)
            add_cost(weight, [a - b for a, b in zip(ahead, moved)])
            if need_grad:
                back = mul_rot_t(ahead, rot)
                for c in range(COMPS):
                    grad[c, pl.ds(v * SUB, SUB), :] = weight * back[c] + prev_col(
                        weight * moved[c]
                    )
            return carry

        lax.fori_loop(0, bands_rows, right_edges, 0)

        def down_edges(v, ahead, weight, push):
            here = block(ys, v, COMPS, t)
            rot = block(down_rot, v, FRAME * FRAME)
            moved = mul_rot(here, rot)
            add_cost(weight, [a - b for a, b in zip(ahead, moved)])
            if need_grad:
                back = mul_rot_t(ahead, rot)
                for c in range(COMPS):
                    grad[c, pl.ds(v * SUB, SUB), :] += weight * back[c]
                    if push:
                        grad[c, pl.ds((v + 1) * SUB, SUB), :] += weight * moved[c]

        def inner_down(v, carry):
            down_edges(v, block(ys, v + 1, COMPS, t), down_wt[pl.ds(v * SUB, SUB), :], True)
            return carry

        lax.fori_loop(0, bands_rows - 1, inner_down, 0)
        top_copy.wait()
        weight = jnp.where(last_band, 0.0, down_wt[end_rows, :])
        down_edges(bands_rows - 1, [top_in[t, c] for c in range(COMPS)], weight, False)
        if need_grad:
            last_copy.wait()
            for c in range(COMPS):
                grad[c, 0:SUB, :] += last_in[t, c]

        near_copy.wait()
        near = [near_in[t, c] for c in range(COMPS)]
        err = [near[c] - src_rot[c] for c in range(COMPS)]
        cost = loop_wt[...] * sum(e * e for e in err)
        sums[t] += sum(cost[k * SUB : (k + 1) * SUB] for k in range(loop_rows // SUB))
        if need_grad:
            back = mul_rot_t(near, [loop_rot[k] for k in range(FRAME * FRAME)])
            for c in range(COMPS):
                vals[c] = loop_wt[...] * back[c]
            scatter(ends.at[0], vals, None, 0)
            src_copy.wait()
            scatter(wanted, src_in, t, loop_rows)
            size = steps[t]

            def update(v, carry):
                here = block(ys, v, COMPS, t)
                pull = block(grad, v, COMPS)
                inner = [
                    [
                        sum(here[i * FRAME + a] * pull[i * FRAME + b] for i in range(LIFTED))
                        for b in range(FRAME)
                    ]
                    for a in range(FRAME)
                ]
                sym = [
                    0.5 * (inner[a][b] + inner[b][a]) for a in range(FRAME) for b in range(FRAME)
                ]
                normal = mul_rot(here, sym)
                new = qf([here[c] + size * (pull[c] - normal[c]) for c in range(COMPS)])
                for c in range(COMPS):
                    ys[t + 1, c, pl.ds(v * SUB, SUB), :] = new[c]
                    if t == iters - 1:
                        out_y[c, pl.ds(v * SUB, SUB), :] = new[c]
                return carry

            lax.fori_loop(0, bands_rows, update, 0)

    rows = [jnp.sum(sums[t], axis=0, keepdims=True) for t in range(iters + 1)]
    tile = jnp.zeros((SUB, LANES), jnp.float32)
    for t in range(iters + 1):
        tile = jnp.where(sub == t, rows[t], tile)
    red_out[0] = tile
    copies = [
        send(red_out.at[0], red_rank.at[d - 1], rank_sem, d - 1, (my_pose, (my_rank + d) % ranks))
        for d in range(1, ranks)
    ]
    for copy in copies:
        copy.wait()
    for d in range(1, ranks):
        tile = tile + red_rank[d - 1]
    red_out[1] = tile
    copies = [
        send(red_out.at[1], red_pose.at[d - 1], pose_sem, d - 1, ((my_pose + d) % poses, my_rank))
        for d in range(1, poses)
    ]
    for copy in copies:
        copy.wait()
    for d in range(1, poses):
        tile = tile + red_pose[d - 1]
    out_cost[...] = scale * jnp.broadcast_to(
        jnp.sum(tile, axis=1, keepdims=True), (SUB, LANES)
    )


def on_device(
    initial, right_rot, right_wt, down_rot, down_wt, loop_ends, loop_rot, loop_wt, step_sizes
):
    pose_dev = initial.shape[2]
    loops = loop_wt.shape[0]
    ranks = lax.axis_size("rank")
    poses = lax.axis_size("pose")
    iters = step_sizes.shape[0]
    prows = pose_dev // LANES
    lrows = loops // LANES
    f32 = jnp.float32
    dma = pltpu.SemaphoreType.DMA
    vmem = pl.BlockSpec(memory_space=pltpu.VMEM)
    out_y, out_cost = pl.pallas_call(
        functools.partial(kernel, ranks, poses, 0.5 / (pose_dev * ranks * poses)),
        out_shape=(
            jax.ShapeDtypeStruct((COMPS, prows, LANES), f32),
            jax.ShapeDtypeStruct((SUB, LANES), f32),
        ),
        in_specs=[vmem] * 8 + [pl.BlockSpec(memory_space=pltpu.SMEM)],
        out_specs=(vmem, vmem),
        scratch_shapes=[
            pltpu.VMEM((iters + 1, COMPS, prows, LANES), f32),
            pltpu.VMEM((lrows, LANES), jnp.int32),
            pltpu.VMEM((iters + 1, COMPS, lrows, LANES), f32),
            pltpu.VMEM((iters + 1, COMPS, lrows, LANES), f32),
            pltpu.VMEM((COMPS, lrows, LANES), f32),
            pltpu.VMEM((iters, COMPS, lrows, LANES), f32),
            pltpu.VMEM((iters, COMPS, lrows, LANES), f32),
            pltpu.VMEM((iters + 1, COMPS, SUB, LANES), f32),
            pltpu.VMEM((iters, COMPS, SUB, LANES), f32),
            pltpu.VMEM((iters, COMPS, SUB, LANES), f32),
            pltpu.VMEM((COMPS, prows, LANES), f32),
            pltpu.VMEM((COMPS, lrows, LANES), f32),
            pltpu.VMEM((COMPS * prows, loops), jnp.bfloat16),
            pltpu.VMEM((2 * LANES, 2 * loops), jnp.bfloat16),
            pltpu.VMEM((iters + 1, SUB, LANES), f32),
            pltpu.VMEM((2, SUB, LANES), f32),
            pltpu.VMEM((ranks - 1, SUB, LANES), f32),
            pltpu.VMEM((poses - 1, SUB, LANES), f32),
            dma((2, 1)),
            dma((2, iters + 1)),
            dma((2, iters)),
            dma((2, iters + 1)),
            dma((2, iters)),
            dma((2, ranks - 1)),
            dma((2, poses - 1)),
        ],
        compiler_params=pltpu.CompilerParams(collective_id=0, has_side_effects=True),
    )(
        initial.reshape(COMPS, prows, LANES),
        right_rot.reshape(FRAME * FRAME, prows, LANES),
        right_wt.reshape(prows, LANES),
        down_rot.reshape(FRAME * FRAME, prows, LANES),
        down_wt.reshape(prows, LANES),
        loop_ends.reshape(2, lrows, LANES),
        loop_rot.reshape(FRAME * FRAME, lrows, LANES),
        loop_wt.reshape(lrows, LANES),
        step_sizes,
    )
    return (out_y.reshape(initial.shape), out_cost[: iters + 1, 0])


def solution(mesh):
    both = ("pose", "rank")
    in_specs = (
        P(None, None, both),
        P(None, None, both),
        P(both),
        P(None, None, both),
        P(both),
        P(None, both),
        P(None, None, both),
        P(both),
        P(),
    )
    out_specs = (P(None, None, both), P())
    return jax.shard_map(
        on_device, mesh=mesh, in_specs=in_specs, out_specs=out_specs, check_vma=False
    )
```

```python
import functools
import jax
import jax.numpy as jnp
from jax import lax
from jax.experimental import pallas as pl
from jax.experimental.pallas import tpu as pltpu
from jax.sharding import PartitionSpec as P

COLS = 1024
LANES = 128
SUB = COLS // LANES
LIFTED = 4
FRAME = 3
COMPS = LIFTED * FRAME
MESH = pl.DeviceIdType.MESH


def mul_rot(y, rot):
    return [
        sum(y[a * LIFTED + i] * rot[a * FRAME + b] for a in range(FRAME))
        for b in range(FRAME)
        for i in range(LIFTED)
    ]


def mul_rot_t(y, rot):
    return [
        sum(y[b * LIFTED + i] * rot[a * FRAME + b] for b in range(FRAME))
        for a in range(FRAME)
        for i in range(LIFTED)
    ]


def qf(y):
    cols = [y[a * LIFTED : (a + 1) * LIFTED] for a in range(FRAME)]

    def unit(col):
        inv = lax.rsqrt(sum(v * v for v in col))
        return [v * inv for v in col]

    def less(col, base):
        along = sum(u * v for u, v in zip(base, col))
        return [v - along * u for u, v in zip(base, col)]

    one = unit(cols[0])
    two = unit(less(cols[1], one))
    three = unit(less(less(cols[2], one), two))
    return one + two + three


def unpack(src, dst, base, rows, lead, width):
    def step(k, carry):
        at = pl.ds(pl.multiple_of(k * LANES, LANES), LANES)
        for a in range(lead):
            piece = src[a, :, at]
            for i in range(width):
                dst[base + a * width + i, pl.ds(k, 1), :] = piece[i : i + 1]
        return carry

    lax.fori_loop(0, rows, step, 0)


def kernel(
    ranks, poses, scale,
    init_in, right_in, right_wt, down_in, down_wt, ends, loop_in, loop_wt, steps,
    out_y, out_cost,
    ys, wanted, near_out, near_in, src_rot, src_out, src_in, top_in, last_out, last_in,
    grad, vals, spread, table, sums, red_out, red_rank, red_pose,
    init, right_rot, down_rot, loop_rot, own_idx, far_idx,
    idx_sem, near_sem, src_sem, top_sem, last_sem, rank_sem, pose_sem,
):
    iters = steps.shape[0]
    pose_rows = init_in.shape[2] // LANES
    bands_rows = pose_rows // SUB
    loop_rows = loop_wt.shape[0]
    half_rows = pose_rows // 2
    my_pose = lax.axis_index("pose")
    my_rank = lax.axis_index("rank")
    bands = ranks * poses
    me = my_pose * ranks + my_rank

    def band(flat):
        return (flat // ranks, flat % ranks)

    partner = band((me + bands // 2) % bands)
    above = band((me + bands - 1) % bands)
    below = band((me + 1) % bands)

    barrier = pltpu.get_barrier_semaphore()
    for target in (partner, above, below):
        pl.semaphore_signal(barrier, inc=1, device_id=target, device_id_type=MESH)
    for d in range(1, ranks):
        pl.semaphore_signal(
            barrier, inc=1, device_id=(my_pose, (my_rank + d) % ranks), device_id_type=MESH
        )
    for d in range(1, poses):
        pl.semaphore_signal(
            barrier, inc=1, device_id=((my_pose + d) % poses, my_rank), device_id_type=MESH
        )
    def send(src, dst, sems, slot, target):
        copy = pltpu.make_async_remote_copy(
            src_ref=src, dst_ref=dst, send_sem=sems.at[0, slot], recv_sem=sems.at[1, slot],
            device_id=target, device_id_type=MESH,
        )
        copy.start()
        return copy

    lane = lax.broadcasted_iota(jnp.int32, (SUB, LANES), 1)
    sub = lax.broadcasted_iota(jnp.int32, (SUB, LANES), 0)
    row_end = (lane == LANES - 1) & (sub == SUB - 1)
    last_band = me == bands - 1

    def block(ref, v, count, lead=None):
        rows = pl.ds(v * SUB, SUB)
        if lead is None:
            return [ref[c, rows, :] for c in range(count)]
        return [ref[lead, c, rows, :] for c in range(count)]

    def next_col(x):
        x = pltpu.roll(x, LANES - 1, 1)
        return jnp.where(lane == LANES - 1, pltpu.roll(x, SUB - 1, 0), x)

    def prev_col(x):
        x = pltpu.roll(x, 1, 1)
        return jnp.where(lane == 0, pltpu.roll(x, 1, 0), x)

    def gather(t, index):
        row = index // LANES
        col = index % LANES

        def step(q, acc):
            acc = list(acc)
            base = pl.multiple_of(q * SUB, SUB)
            for j in range(SUB):
                hit = row == q * SUB + j
                for c in range(COMPS):
                    data = jnp.broadcast_to(ys[t, c, pl.ds(base + j, 1), :], (SUB, LANES))
                    got = jnp.take_along_axis(data, col, axis=1, mode="promise_in_bounds")
                    acc[c] = jnp.where(hit, got, acc[c])
            return tuple(acc)

        zero = jnp.zeros((SUB, LANES), jnp.float32)
        return lax.fori_loop(0, pose_rows // SUB, step, (zero,) * COMPS)

    def fill_table(index_ref, base):
        def step(k, carry):
            index = index_ref[pl.ds(k, 1), :]
            low = (index // (half_rows * LANES)) * LANES + index % LANES
            place = lax.broadcasted_iota(jnp.int32, (2 * LANES, LANES), 0)
            hot = jnp.where(place == low, 1.0, 0.0).astype(jnp.bfloat16)
            table[:, pl.ds(pl.multiple_of((base + k) * LANES, LANES), LANES)] = hot
            return carry

        lax.fori_loop(0, loop_rows, step, 0)

    def scatter(index_ref, values, h, base):
        def step(k, carry):
            index = index_ref[pl.ds(h * SUB + k, 1), :]
            high = (index // LANES) % half_rows
            hit = lax.broadcasted_iota(jnp.int32, (half_rows, LANES), 0) == high
            at = pl.ds(pl.multiple_of(k * LANES, LANES), LANES)
            for c in range(COMPS):
                value = values(c, k)
                coarse = value.astype(jnp.bfloat16).astype(jnp.float32)
                fine = value - coarse
                spread[pl.ds(c * half_rows, half_rows), at] = jnp.where(
                    hit, coarse, 0.0
                ).astype(jnp.bfloat16)
                spread[pl.ds((COMPS + c) * half_rows, half_rows), at] = jnp.where(
                    hit, fine, 0.0
                ).astype(jnp.bfloat16)
            return carry

        lax.fori_loop(0, SUB, step, 0)
        start = (base + h * SUB) * LANES
        placed = lax.dot_general(
            spread[...], table[:, start : start + SUB * LANES],
            (((1,), (1,)), ((), ())), preferred_element_type=jnp.float32,
        )
        for c in range(COMPS):
            both = (
                placed[c * half_rows : (c + 1) * half_rows]
                + placed[(COMPS + c) * half_rows : (COMPS + c + 1) * half_rows]
            )
            for g in range(2):
                grad[c, g * half_rows : (g + 1) * half_rows, :] += both[
                    :, g * LANES : (g + 1) * LANES
                ]

    def spread_index(src, dst):
        for k in range(loop_rows):
            for e in range(2):
                dst[e, k : k + 1, :] = src[e : e + 1, k * LANES : (k + 1) * LANES]

    def first(v, carry):
        new = qf(block(init, v, COMPS))
        for c in range(COMPS):
            ys[0, c, pl.ds(v * SUB, SUB), :] = new[c]
        return carry

    unpack(init_in, init, 0, pose_rows, FRAME, LIFTED)
    lax.fori_loop(0, bands_rows, first, 0)
    spread_index(ends, own_idx)
    unpack(loop_in, loop_rot, 0, loop_rows, FRAME, FRAME)
    pl.semaphore_wait(barrier, 3 + ranks - 1 + poses - 1)
    idx_copy = send(ends, wanted, idx_sem, 0, partner)
    chunks = loop_rows // SUB
    end_rows = pl.ds((bands_rows - 1) * SUB, SUB)
    for t in range(iters + 1):
        need_grad = t < iters
        near_copy = []
        src_copy = []

        def send_near():
            for h in range(chunks):
                got = gather(t, far_idx[1, h * SUB : (h + 1) * SUB])
                for c in range(COMPS):
                    near_out[t, h, c] = got[c]
                near_copy.append(
                    send(near_out.at[t, h], near_in.at[t, h], near_sem, t * chunks + h, partner)
                )

        def send_src():
            for h in range(chunks):
                rows = slice(h * SUB, (h + 1) * SUB)
                got = gather(t, own_idx[0, rows])
                turned = mul_rot(got, [loop_rot[k, rows] for k in range(FRAME * FRAME)])
                for c in range(COMPS):
                    src_rot[h, c] = turned[c]
                if need_grad:
                    weight = loop_wt[rows]
                    for c in range(COMPS):
                        src_out[t, h, c] = weight * turned[c]
                    src_copy.append(
                        send(src_out.at[t, h], src_in.at[t, h], src_sem, t * chunks + h, partner)
                    )

        top_copy = send(ys.at[t, :, pl.ds(0, SUB), :], top_in.at[t], top_sem, t, above)
        if t == 0:
            send_src()
            idx_copy.wait()
            spread_index(wanted, far_idx)
            send_near()
            unpack(down_in, down_rot, 0, pose_rows, FRAME, FRAME)
        else:
            send_near()
            send_src()
        if need_grad:
            rot = block(down_rot, bands_rows - 1, FRAME * FRAME)
            weight = jnp.where(last_band, 0.0, down_wt[end_rows, :])
            turned = mul_rot(block(ys, bands_rows - 1, COMPS, t), rot)
            for c in range(COMPS):
                last_out[t, c] = weight * turned[c]
            last_copy = send(last_out.at[t], last_in.at[t], last_sem, t, below)
        if t == 0:
            unpack(right_in, right_rot, 0, pose_rows, FRAME, FRAME)
            fill_table(own_idx.at[0], 0)
            fill_table(far_idx.at[1], loop_rows)
        if t == iters:

            def repack(k, carry):
                at = pl.ds(pl.multiple_of(k * LANES, LANES), LANES)
                for a in range(FRAME):
                    for i in range(LIFTED):
                        out_y[a, i : i + 1, at] = ys[t, a * LIFTED + i, pl.ds(k, 1), :]
                return carry

            lax.fori_loop(0, pose_rows, repack, 0)

        def add_cost(weight, err):
            sums[t] += weight * sum(e * e for e in err)

        sums[t] = jnp.zeros((SUB, LANES), jnp.float32)

        def right_edges(v, carry):
            here = block(ys, v, COMPS, t)
            rot = block(right_rot, v, FRAME * FRAME)
            weight = jnp.where(row_end, 0.0, right_wt[pl.ds(v * SUB, SUB), :])
            ahead = [next_col(x) for x in here]
            moved = mul_rot(here, rot)
            add_cost(weight, [a - b for a, b in zip(ahead, moved)])
            if need_grad:
                back = mul_rot_t(ahead, rot)
                for c in range(COMPS):
                    grad[c, pl.ds(v * SUB, SUB), :] = weight * back[c] + prev_col(
                        weight * moved[c]
                    )
            return carry

        lax.fori_loop(0, bands_rows, right_edges, 0)

        def down_edges(v, ahead, weight, push):
            here = block(ys, v, COMPS, t)
            rot = block(down_rot, v, FRAME * FRAME)
            moved = mul_rot(here, rot)
            add_cost(weight, [a - b for a, b in zip(ahead, moved)])
            if need_grad:
                back = mul_rot_t(ahead, rot)
                for c in range(COMPS):
                    grad[c, pl.ds(v * SUB, SUB), :] += weight * back[c]
                    if push:
                        grad[c, pl.ds((v + 1) * SUB, SUB), :] += weight * moved[c]

        def inner_down(v, carry):
            down_edges(v, block(ys, v + 1, COMPS, t), down_wt[pl.ds(v * SUB, SUB), :], True)
            return carry

        lax.fori_loop(0, bands_rows - 1, inner_down, 0)
        top_copy.wait()
        weight = jnp.where(last_band, 0.0, down_wt[end_rows, :])
        down_edges(bands_rows - 1, [top_in[t, c] for c in range(COMPS)], weight, False)
        if need_grad:
            last_copy.wait()
            for c in range(COMPS):
                grad[c, 0:SUB, :] += last_in[t, c]

        def take_near():
            for h in range(chunks):
                rows = slice(h * SUB, (h + 1) * SUB)
                near_copy[h].wait()
                near = [near_in[t, h, c] for c in range(COMPS)]
                weight = loop_wt[rows]
                add_cost(weight, [near[c] - src_rot[h, c] for c in range(COMPS)])
                if need_grad:
                    back = mul_rot_t(near, [loop_rot[k, rows] for k in range(FRAME * FRAME)])
                    for c in range(COMPS):
                        vals[h, c] = weight * back[c]
                    scatter(own_idx.at[0], lambda c, k: vals[h, c, pl.ds(k, 1), :], h, 0)

        def take_src():
            for h in range(chunks):
                src_copy[h].wait()
                scatter(
                    far_idx.at[1], lambda c, k: src_in[t, h, c, pl.ds(k, 1), :], h, loop_rows
                )

        if t == 0:
            take_src()
            take_near()
        else:
            take_near()
            if need_grad:
                take_src()
        if need_grad:
            size = steps[t]

            def update(v, carry):
                here = block(ys, v, COMPS, t)
                pull = block(grad, v, COMPS)
                inner = [
                    [
                        sum(here[a * LIFTED + i] * pull[b * LIFTED + i] for i in range(LIFTED))
                        for b in range(FRAME)
                    ]
                    for a in range(FRAME)
                ]
                sym = [
                    0.5 * (inner[a][b] + inner[b][a]) for a in range(FRAME) for b in range(FRAME)
                ]
                normal = mul_rot(here, sym)
                new = qf([here[c] + size * (pull[c] - normal[c]) for c in range(COMPS)])
                for c in range(COMPS):
                    ys[t + 1, c, pl.ds(v * SUB, SUB), :] = new[c]
                return carry

            lax.fori_loop(0, bands_rows, update, 0)

    rows = [jnp.sum(sums[t], axis=0, keepdims=True) for t in range(iters + 1)]
    tile = jnp.zeros((SUB, LANES), jnp.float32)
    for t in range(iters + 1):
        tile = jnp.where(sub == t, rows[t], tile)
    red_out[0] = tile
    copies = [
        send(red_out.at[0], red_rank.at[d - 1], rank_sem, d - 1, (my_pose, (my_rank + d) % ranks))
        for d in range(1, ranks)
    ]
    for copy in copies:
        copy.wait()
    for d in range(1, ranks):
        tile = tile + red_rank[d - 1]
    red_out[1] = tile
    copies = [
        send(red_out.at[1], red_pose.at[d - 1], pose_sem, d - 1, ((my_pose + d) % poses, my_rank))
        for d in range(1, poses)
    ]
    for copy in copies:
        copy.wait()
    for d in range(1, poses):
        tile = tile + red_pose[d - 1]
    for t in range(iters + 1):
        out_cost[t] = scale * jnp.sum(tile[t : t + 1])


def on_device(
    initial, right_rot, right_wt, down_rot, down_wt, loop_ends, loop_rot, loop_wt, step_sizes
):
    pose_dev = initial.shape[2]
    loops = loop_wt.shape[0]
    ranks = lax.axis_size("rank")
    poses = lax.axis_size("pose")
    iters = step_sizes.shape[0]
    prows = pose_dev // LANES
    lrows = loops // LANES
    chunks = lrows // SUB
    f32 = jnp.float32
    dma = pltpu.SemaphoreType.DMA
    vmem = pl.BlockSpec(memory_space=pltpu.VMEM)
    out_y, out_cost = pl.pallas_call(
        functools.partial(kernel, ranks, poses, 0.5 / (pose_dev * ranks * poses)),
        out_shape=(
            jax.ShapeDtypeStruct((FRAME, LIFTED, pose_dev), f32),
            jax.ShapeDtypeStruct((iters + 1,), f32),
        ),
        in_specs=[vmem] * 8 + [pl.BlockSpec(memory_space=pltpu.SMEM)],
        out_specs=(vmem, pl.BlockSpec(memory_space=pltpu.SMEM)),
        scratch_shapes=[
            pltpu.VMEM((iters + 1, COMPS, prows, LANES), f32),
            pltpu.VMEM((2, loops), jnp.int32),
            pltpu.VMEM((iters + 1, chunks, COMPS, SUB, LANES), f32),
            pltpu.VMEM((iters + 1, chunks, COMPS, SUB, LANES), f32),
            pltpu.VMEM((chunks, COMPS, SUB, LANES), f32),
            pltpu.VMEM((iters, chunks, COMPS, SUB, LANES), f32),
            pltpu.VMEM((iters, chunks, COMPS, SUB, LANES), f32),
            pltpu.VMEM((iters + 1, COMPS, SUB, LANES), f32),
            pltpu.VMEM((iters, COMPS, SUB, LANES), f32),
            pltpu.VMEM((iters, COMPS, SUB, LANES), f32),
            pltpu.VMEM((COMPS, prows, LANES), f32),
            pltpu.VMEM((chunks, COMPS, SUB, LANES), f32),
            pltpu.VMEM((COMPS * prows, SUB * LANES), jnp.bfloat16),
            pltpu.VMEM((2 * LANES, 2 * loops), jnp.bfloat16),
            pltpu.VMEM((iters + 1, SUB, LANES), f32),
            pltpu.VMEM((2, SUB, LANES), f32),
            pltpu.VMEM((ranks - 1, SUB, LANES), f32),
            pltpu.VMEM((poses - 1, SUB, LANES), f32),
            pltpu.VMEM((COMPS, prows, LANES), f32),
            pltpu.VMEM((FRAME * FRAME, prows, LANES), f32),
            pltpu.VMEM((FRAME * FRAME, prows, LANES), f32),
            pltpu.VMEM((FRAME * FRAME, lrows, LANES), f32),
            pltpu.VMEM((2, lrows, LANES), jnp.int32),
            pltpu.VMEM((2, lrows, LANES), jnp.int32),
            dma((2, 1)),
            dma((2, (iters + 1) * chunks)),
            dma((2, iters * chunks)),
            dma((2, iters + 1)),
            dma((2, iters)),
            dma((2, ranks - 1)),
            dma((2, poses - 1)),
        ],
        compiler_params=pltpu.CompilerParams(collective_id=0, has_side_effects=True),
    )(
        jnp.transpose(initial, (1, 0, 2)),
        right_rot,
        right_wt.reshape(prows, LANES),
        down_rot,
        down_wt.reshape(prows, LANES),
        loop_ends,
        loop_rot,
        loop_wt.reshape(lrows, LANES),
        step_sizes,
    )
    return (jnp.transpose(out_y, (1, 0, 2)), out_cost)


def solution(mesh):
    both = ("pose", "rank")
    in_specs = (
        P(None, None, both),
        P(None, None, both),
        P(both),
        P(None, None, both),
        P(both),
        P(None, both),
        P(None, None, both),
        P(both),
        P(),
    )
    out_specs = (P(None, None, both), P())
    return jax.shard_map(
        on_device, mesh=mesh, in_specs=in_specs, out_specs=out_specs, check_vma=False
    )
```
